8 devices in a mesh: dp: 2 (over z, y), cp: 4 (over x, core).
Axes of the slice: x: 2, y: 2, z: 1, core: 2. Of those that a mesh axis runs over, the one named last changes fastest.
Arguments:
- hidden: bfloat16 [24, 768, 7168], P('dp', 'cp')
- positions: int32 [768], P('cp')
- w_q: bfloat16 [7168, 8192], replicated
- w_k: bfloat16 [7168, 8192], replicated
- w_v: bfloat16 [7168, 8192], replicated
- w_o: bfloat16 [8192, 7168], replicated
Outputs:
- output 1: bfloat16 [24, 768, 7168], P('dp', 'cp')
- output 2: float32 [64], replicated
- output 3: bfloat16 [7168, 8192], replicated
- output 4: bfloat16 [7168, 8192], replicated
All inputs are finite; a program needn't handle non-finite values.
Results may differ from the reference program's by a relative error of at most 0.00749088.
Values are sent between devices in bfloat16 or wider.
A program may use at most 3 GiB of HBM per device.

```python
import jax
import jax.numpy as jnp
from jax import lax

BATCH_SIZE = 24
SEQ_LEN = 768
D_MODEL = 7168
NUM_HEADS = 64
QUERY_BLOCK = 64
HEAD_DIM = 128
TAU_CLIP = 100
ROPE_THETA = 50000


def rope_rotate(tensor, pos_ids):
    half_dim = HEAD_DIM // 2
    inv_freq = jnp.float32(ROPE_THETA) ** (-jnp.arange(half_dim, dtype=jnp.float32) * (2.0 / HEAD_DIM))
    angle = pos_ids.astype(jnp.float32)[:, None] * inv_freq[None, :]
    cos_t = jnp.cos(angle)[:, None, :]
    sin_t = jnp.sin(angle)[:, None, :]
    lead_half = tensor[..., :half_dim]
    tail_half = tensor[..., half_dim:]
    return jnp.concatenate([lead_half * cos_t - tail_half * sin_t, tail_half * cos_t + lead_half * sin_t], axis=-1)


def setup_inputs(seed: int = 0) -> dict:
    root_key = jax.random.key(seed)
    sub_keys = jax.random.split(root_key, 15)
    width = NUM_HEADS * HEAD_DIM
    gaps = jax.random.randint(sub_keys[0], (SEQ_LEN,), 1, 3)
    start_pos = jax.random.randint(sub_keys[1], (), 0, SEQ_LEN // 2 + 1)
    positions = (start_pos + jnp.cumsum(gaps) - 1).astype(jnp.int32)
    spike_row = jax.random.randint(sub_keys[2], (), 0, BATCH_SIZE)
    key_slot = jax.random.randint(sub_keys[3], (), 0, SEQ_LEN // 2)
    query_slot = jax.random.randint(sub_keys[4], (), SEQ_LEN // 2, SEQ_LEN)
    clip_heads = (jax.random.permutation(sub_keys[5], NUM_HEADS) < NUM_HEADS // 2).astype(jnp.float32)
    head_gain = jax.random.uniform(sub_keys[6], (NUM_HEADS,), jnp.float32, 1.0, 1.25)
    dir_query = jax.random.normal(sub_keys[7], (D_MODEL,), jnp.float32)
    dir_query = dir_query / jnp.sqrt(jnp.sum(dir_query * dir_query))
    dir_key = jax.random.normal(sub_keys[8], (D_MODEL,), jnp.float32)
    dir_key = dir_key / jnp.sqrt(jnp.sum(dir_key * dir_key))
    plant_q = jax.random.normal(sub_keys[9], (NUM_HEADS, HEAD_DIM), jnp.float32)
    plant_q = plant_q / jnp.sqrt(jnp.mean(plant_q * plant_q, axis=-1, keepdims=True))
    plant_q = plant_q * (4.0 * head_gain * clip_heads)[:, None] * D_MODEL ** -0.5
    delta = positions[query_slot] - positions[key_slot]
    plant_k = rope_rotate(plant_q[None], delta[None])[0]
    noise_scale = 1.5 * D_MODEL ** -0.5
    w_q = noise_scale * jax.random.normal(sub_keys[10], (D_MODEL, width), jnp.float32) + dir_query[:, None] * plant_q.reshape(width)[None, :]
    w_k = noise_scale * jax.random.normal(sub_keys[11], (D_MODEL, width), jnp.float32) + dir_key[:, None] * plant_k.reshape(width)[None, :]
    w_v = jax.random.normal(sub_keys[12], (D_MODEL, width), jnp.float32) * D_MODEL ** -0.5
    w_o = jax.random.normal(sub_keys[13], (width, D_MODEL), jnp.float32) * width ** -0.5
    hidden = jax.random.normal(sub_keys[14], (BATCH_SIZE, SEQ_LEN, D_MODEL), jnp.float32)
    spike_scale = jnp.sqrt(jnp.float32(D_MODEL))
    hidden = hidden.at[spike_row, query_slot].set(spike_scale * dir_query)
    hidden = hidden.at[spike_row, key_slot].set(spike_scale * dir_key)
    return {
        "hidden": hidden.astype(jnp.bfloat16),
        "positions": positions,
        "w_q": w_q.astype(jnp.bfloat16),
        "w_k": w_k.astype(jnp.bfloat16),
        "w_v": w_v.astype(jnp.bfloat16),
        "w_o": w_o.astype(jnp.bfloat16),
    }


def reference(hidden, positions, w_q, w_k, w_v, w_o):
    score_scale = HEAD_DIM ** -0.5
    n_blocks = SEQ_LEN // QUERY_BLOCK
    pos_blocks = positions.reshape(n_blocks, QUERY_BLOCK)
    head_shape = (SEQ_LEN, NUM_HEADS, HEAD_DIM)

    def one_row(row_in):
        q_all = rope_rotate(jnp.dot(row_in, w_q, preferred_element_type=jnp.float32).reshape(head_shape), positions).astype(jnp.bfloat16)
        k_all = rope_rotate(jnp.dot(row_in, w_k, preferred_element_type=jnp.float32).reshape(head_shape), positions).astype(jnp.bfloat16)
        v_all = jnp.dot(row_in, w_v, preferred_element_type=jnp.float32).astype(jnp.bfloat16).reshape(head_shape)
        k_wide = k_all.astype(jnp.float32)
        v_wide = v_all.astype(jnp.float32)
        q_blocks = q_all.reshape(n_blocks, QUERY_BLOCK, NUM_HEADS, HEAD_DIM)

        def one_block(block_in):
            q_blk, pos_blk = block_in
            scores = jnp.einsum("qhd,khd->hqk", q_blk.astype(jnp.float32), k_wide) * score_scale
            allowed = positions[None, None, :] <= pos_blk[None, :, None]
            scores = jnp.where(allowed, scores, -jnp.inf)
            block_max = jnp.max(scores, axis=(1, 2))
            prob_w = jax.nn.softmax(scores, axis=-1)
            attn_blk = jnp.einsum("hqk,khd->qhd", prob_w, v_wide)
            return attn_blk.astype(jnp.bfloat16), block_max

        attn_blocks, block_maxes = lax.map(one_block, (q_blocks, pos_blocks))
        attn_flat = attn_blocks.reshape(SEQ_LEN, NUM_HEADS * HEAD_DIM)
        row_out = jnp.dot(attn_flat, w_o, preferred_element_type=jnp.float32).astype(jnp.bfloat16)
        return row_out, jnp.max(block_maxes, axis=0)

    attn_out, row_maxes = lax.map(one_row, hidden)
    head_max = jnp.max(row_maxes, axis=0)
    factor = jnp.where(head_max > TAU_CLIP, jnp.sqrt(TAU_CLIP / head_max), 1.0)
    col_factor = jnp.repeat(factor, HEAD_DIM)
    w_q_new = (w_q.astype(jnp.float32) * col_factor[None, :]).astype(jnp.bfloat16)
    w_k_new = (w_k.astype(jnp.float32) * col_factor[None, :]).astype(jnp.bfloat16)
    return attn_out, head_max, w_q_new, w_k_new
```

```python
import functools

import jax
import jax.numpy as jnp
from jax import lax
from jax.experimental import pallas as pl
from jax.experimental.pallas import tpu as pltpu
from jax.sharding import PartitionSpec as P


HEAD_DIM = 128
TAU_CLIP = 100.0
ROPE_THETA = 50000.0
LOG2_E = 1.4426950408889634
SCALE = HEAD_DIM ** -0.5
MIB = 1024 * 1024
BF16 = jnp.bfloat16
F32 = jnp.float32
ANY = pl.BlockSpec(memory_space=pl.ANY)


def params(mib=60, **kw):
    return pltpu.CompilerParams(vmem_limit_bytes=mib * MIB, dimension_semantics=("arbitrary",), **kw)


def cost(flops, nbytes):
    return pl.CostEstimate(flops=int(flops), bytes_accessed=int(nbytes), transcendentals=0)


def gather_kernel(axes, src, out, send_sems, recv_sems):
    sizes = [n for _, n in axes]
    me = [lax.axis_index(a) for a, _ in axes]
    total = 1
    for n in sizes:
        total *= n
    my_slot = 0
    for i, n in zip(me, sizes):
        my_slot = my_slot * n + i
    shifts = []
    for lin in range(1, total):
        rest, sh = lin, []
        for n in reversed(sizes):
            sh.insert(0, rest % n)
            rest //= n
        shifts.append(sh)

    def peer(sh):
        return {a: lax.rem(i + d, n) for (a, n), i, d in zip(axes, me, sh)}

    barrier = pltpu.get_barrier_semaphore()
    for sh in shifts:
        pl.semaphore_signal(barrier, inc=1, device_id=peer(sh), device_id_type=pl.DeviceIdType.MESH)
    pl.semaphore_wait(barrier, total - 1)
    copies = []
    for j, sh in enumerate(shifts):
        copy = pltpu.make_async_remote_copy(
            src_ref=src, dst_ref=out.at[my_slot], send_sem=send_sems.at[j], recv_sem=recv_sems.at[j],
            device_id=peer(sh), device_id_type=pl.DeviceIdType.MESH)
        copy.start()
        copies.append(copy)
    out[my_slot] = src[...]
    for copy in copies:
        copy.wait()


def gather_small(x, axes, collective_id):
    total = 1
    for _, n in axes:
        total *= n
    return pl.pallas_call(
        functools.partial(gather_kernel, axes),
        out_shape=jax.ShapeDtypeStruct((total,) + x.shape, x.dtype),
        in_specs=[pl.BlockSpec(memory_space=pltpu.VMEM)],
        out_specs=pl.BlockSpec(memory_space=pltpu.VMEM),
        scratch_shapes=[pltpu.SemaphoreType.DMA((total - 1,)), pltpu.SemaphoreType.DMA((total - 1,))],
        compiler_params=pltpu.CompilerParams(collective_id=collective_id, has_side_effects=True),
        name="gather_small",
    )(x)


def proj_kernel(rows, where, xa, xb, wq, wk, wv, cos, sin, *rest):
    q_out, k_out, v_out, xs, sems = rest[-5:]
    r0, nr = rows
    seq = xs.shape[2]

    @pl.when(pl.program_id(0) == 0)
    def _():
        ca = pltpu.make_async_copy(xa.at[pl.ds(where[1] + r0, nr)], xs.at[:, where[3]], sems.at[0])
        cb = pltpu.make_async_copy(xb.at[pl.ds(where[2] + r0, nr)], xs.at[:, 1 - where[3]], sems.at[1])
        ca.start()
        cb.start()
        ca.wait()
        cb.wait()

    x = xs[...].reshape(nr * 2 * seq, xs.shape[3])
    half = 2 * seq
    cos_t = cos[...]
    sin_t = sin[...]

    def rotated(t, out):
        for r in range(nr):
            for j in range(t.shape[1] // HEAD_DIM):
                h = t[r * half:(r + 1) * half, j * HEAD_DIM:(j + 1) * HEAD_DIM]
                turned = h * cos_t + pltpu.roll(h, HEAD_DIM // 2, 1) * sin_t
                out[r, 0, :, j * HEAD_DIM:(j + 1) * HEAD_DIM] = turned.astype(BF16)

    rotated(jnp.dot(x, wq[...], preferred_element_type=F32), q_out)
    rotated(jnp.dot(x, wk[...], preferred_element_type=F32), k_out)
    v = jnp.dot(x, wv[...], preferred_element_type=F32).astype(BF16)
    for r in range(nr):
        v_out[r, 0] = v[r * half:(r + 1) * half]


def project(xa, xb, where, rows, w_q, w_k, w_v, cos, sin, qkv=None, qkv_shape=None):
    r0, nr = rows
    dim, width = w_q.shape
    seq = xa.shape[1]
    bn = min(256, width)
    half = 2 * seq
    w_spec = pl.BlockSpec((dim, bn), lambda n, w: (0, n))
    t_spec = pl.BlockSpec((half, HEAD_DIM), lambda n, w: (w[0], 0), pipeline_mode=pl.Buffered(buffer_count=1))
    assert r0 % nr == 0
    o_spec = pl.BlockSpec((nr, 1, half, bn), lambda n, w: (r0 // nr, w[0], 0, n))
    old = [] if qkv is None else list(qkv)
    shape = qkv_shape if qkv is None else qkv[0].shape
    tokens = nr * half
    return pl.pallas_call(
        functools.partial(proj_kernel, rows),
        grid_spec=pltpu.PrefetchScalarGridSpec(
            num_scalar_prefetch=1, grid=(width // bn,),
            in_specs=[ANY, ANY, w_spec, w_spec, w_spec, t_spec, t_spec] + [ANY] * len(old),
            out_specs=[o_spec] * 3,
            scratch_shapes=[pltpu.VMEM((nr, 2, seq, dim), BF16), pltpu.SemaphoreType.DMA((2,))]),
        out_shape=[jax.ShapeDtypeStruct(shape, BF16)] * 3,
        input_output_aliases={8 + i: i for i in range(len(old))},
        compiler_params=params(),
        cost_estimate=cost(6 * tokens * dim * width, 6 * dim * width + 2 * tokens * (dim + 3 * width)),
        name="project",
    )(where, xa, xb, w_q, w_k, w_v, cos, sin, *old)


def attend_kernel(q, k, v, out, peak):
    s_len = 2 * q.shape[2]
    bq = 256
    for j in range(q.shape[3] // HEAD_DIM):
        cols = slice(j * HEAD_DIM, (j + 1) * HEAD_DIM)
        qh = q[0, :, :, cols].reshape(s_len, HEAD_DIM)
        kh = k[0, :, :, cols].reshape(s_len, HEAD_DIM)
        vh = v[0, :, :, cols].reshape(s_len, HEAD_DIM)
        best = None
        for i in range(s_len // bq):
            lo, hi = i * bq, (i + 1) * bq
            s = lax.dot_general(qh[lo:hi], kh[:hi], (((1,), (1,)), ((), ())), preferred_element_type=F32)
            keep = lax.broadcasted_iota(jnp.int32, (bq, bq), 0) >= lax.broadcasted_iota(jnp.int32, (bq, bq), 1)
            diag = jnp.where(keep, s[:, lo:], -jnp.inf)
            s = diag if i == 0 else jnp.concatenate([s[:, :lo], diag], axis=1)
            m = jnp.max(s, axis=1, keepdims=True)
            best = m if best is None else jnp.maximum(best, m)
            p = jnp.exp2((s - m) * (SCALE * LOG2_E))
            total = jnp.sum(p, axis=1, keepdims=True)
            o = jnp.dot(p.astype(BF16), vh[:hi], preferred_element_type=F32)
            out[0, lo:hi, cols] = (o / total).astype(BF16)
        peak[0, j:j + 1] = jnp.broadcast_to(jnp.max(best, axis=0, keepdims=True), (1, HEAD_DIM))


def attend(qkv, row, out=None):
    q, k, v = qkv
    rows, _, half, width = q.shape
    bn = min(256, width)
    spec = pl.BlockSpec((1, 2, half, bn), lambda n: (row, 0, 0, n))
    steps = width // bn
    kernel = attend_kernel if out is None else lambda q, k, v, old, out, peak: attend_kernel(q, k, v, out, peak)
    old = [] if out is None else [out]
    pairs = 2 * half * 2 * half
    return pl.pallas_call(
        kernel,
        grid=(steps,),
        in_specs=[spec] * 3 + [ANY] * len(old),
        out_specs=[pl.BlockSpec((1, 2 * half, bn), lambda n: (row, 0, n)), pl.BlockSpec((1, 8, HEAD_DIM), lambda n: (n, 0, 0))],
        out_shape=[jax.ShapeDtypeStruct((rows, 2 * half, width), BF16), jax.ShapeDtypeStruct((steps, 8, HEAD_DIM), F32)],
        input_output_aliases={3: 0} if old else {},
        compiler_params=params(),
        cost_estimate=cost(8 * pairs * width, 8 * 2 * half * width),
        name="attend",
    )(q, k, v, *old)


def load_tokens(pieces, attn, xs, sems):
    copies = [pltpu.make_async_copy(attn.at[r, p], xs.at[i], sems.at[i]) for i, (r, p) in enumerate(pieces)]
    for c in copies:
        c.start()
    for c in copies:
        c.wait()


def out_far_kernel(row, clip, where, attn, w_o, *rest):
    if clip:
        w_in, factor, o2, o3, o1, w_new, xs, sems = rest
    else:
        o2, o3, o1, xs, sems = rest

    @pl.when(pl.program_id(0) == 0)
    def _():
        load_tokens([(row, where[2]), (row, where[3]), (row, where[1])], attn, xs, sems)

    n_pieces, seq, width = xs.shape
    y = jnp.dot(xs[...].reshape(n_pieces * seq, width), w_o[...], preferred_element_type=F32).astype(BF16)
    o2[...] = y[:seq]
    o3[...] = y[seq:2 * seq]
    o1[...] = y[2 * seq:]
    if clip:
        w_new[...] = (w_in[...].astype(F32) * factor[...]).astype(BF16)


def out_far(attn, w_o, where, row, clip=None):
    _, _, seq, width = attn.shape
    dim = w_o.shape[1]
    bn = min(512, dim) if clip is None else min(256, dim)
    steps = dim // bn
    o_spec = pl.BlockSpec((seq, bn), lambda n, w: (0, n))
    in_specs = [ANY, pl.BlockSpec((width, bn), lambda n, w: (0, n))]
    out_specs = [o_spec] * 3
    out_shape = [jax.ShapeDtypeStruct((seq, dim), BF16)] * 3
    args = [attn, w_o]
    if clip is not None:
        w_in, factor = clip
        c_spec = pl.BlockSpec((w_in.shape[0] // steps, width), lambda n, w: (n, 0))
        in_specs += [c_spec, pl.BlockSpec((1, width), lambda n, w: (0, 0))]
        out_specs = out_specs + [c_spec]
        out_shape = out_shape + [jax.ShapeDtypeStruct(w_in.shape, BF16)]
        args += [w_in, factor]
    return pl.pallas_call(
        functools.partial(out_far_kernel, row, clip is not None),
        grid_spec=pltpu.PrefetchScalarGridSpec(
            num_scalar_prefetch=1, grid=(steps,), in_specs=in_specs, out_specs=out_specs,
            scratch_shapes=[pltpu.VMEM((3, seq, width), BF16), pltpu.SemaphoreType.DMA((3,))]),
        out_shape=out_shape,
        compiler_params=params(),
        cost_estimate=cost(6 * seq * dim * width, 2 * dim * width + 6 * seq * (dim + width)),
        name="out_far",
    )(where, *args)


def out_own_kernel(where, attn, w_o, w_in, factor, out, w_new, xs, sems):
    @pl.when(pl.program_id(0) == 0)
    def _():
        load_tokens([(r, where[0]) for r in range(xs.shape[0])], attn, xs, sems)

    n_pieces, seq, width = xs.shape
    y = jnp.dot(xs[...].reshape(n_pieces * seq, width), w_o[...], preferred_element_type=F32).astype(BF16)
    out[...] = y.reshape(n_pieces, seq, y.shape[1])
    w_new[...] = (w_in[...].astype(F32) * factor[...]).astype(BF16)


def out_own(attn, w_o, where, batch, w_in, factor):
    rows, _, seq, width = attn.shape
    dim = w_o.shape[1]
    bn = min(256, dim)
    steps = dim // bn
    c_spec = pl.BlockSpec((w_in.shape[0] // steps, width), lambda n, w: (n, 0))
    return pl.pallas_call(
        out_own_kernel,
        grid_spec=pltpu.PrefetchScalarGridSpec(
            num_scalar_prefetch=1, grid=(steps,),
            in_specs=[ANY, pl.BlockSpec((width, bn), lambda n, w: (0, n)), c_spec, pl.BlockSpec((1, width), lambda n, w: (0, 0))],
            out_specs=[pl.BlockSpec((rows, seq, bn), lambda n, w: (w[0], 0, n)), c_spec],
            scratch_shapes=[pltpu.VMEM((rows, seq, width), BF16), pltpu.SemaphoreType.DMA((rows,))]),
        out_shape=[jax.ShapeDtypeStruct((batch, seq, dim), BF16), jax.ShapeDtypeStruct(w_in.shape, BF16)],
        compiler_params=params(),
        cost_estimate=cost(2 * rows * seq * dim * width, 6 * dim * width),
        name="out_own",
    )(where, attn, w_o, w_in, factor)


def rope_tables(pos_ids):
    half_dim = HEAD_DIM // 2
    inv_freq = jnp.float32(ROPE_THETA) ** (-jnp.arange(half_dim, dtype=F32) * (2.0 / HEAD_DIM))
    angle = pos_ids.astype(F32)[:, None] * inv_freq[None, :]
    cos_t, sin_t = jnp.cos(angle), jnp.sin(angle)
    return jnp.concatenate([cos_t, cos_t], axis=1), jnp.concatenate([-sin_t, sin_t], axis=1)


def solution(mesh):
    cp_size = mesh.shape["cp"]
    dp_size = mesh.shape["dp"]
    assert cp_size == 4
    swaps = {s: [(i, i ^ s) for i in range(cp_size)] for s in (1, 2, 3)}

    def compute(hidden, pos_ids, w_q, w_k, w_v, w_o):
        batch, seq, _ = hidden.shape
        width = w_q.shape[1]
        rows = batch // cp_size
        cp = lax.axis_index("cp").astype(jnp.int32)
        chip, core = cp // 2, cp % 2

        def outgoing(s):
            return lax.dynamic_slice_in_dim(hidden, (cp ^ s) * rows, rows, axis=0)

        got = {s: lax.ppermute(outgoing(s), "cp", swaps[s]) for s in (2, 3, 1)}

        pos_block = jnp.zeros((8, 256), jnp.int32).at[0, :seq].set(pos_ids)
        all_pos = gather_small(pos_block, (("cp", cp_size),), 0)[:, 0, :seq].reshape(cp_size * seq)
        cos, sin = rope_tables(all_pos)

        near = jnp.stack([chip, cp * rows, jnp.zeros_like(cp), core]).astype(jnp.int32)
        far = jnp.stack([1 - chip, jnp.zeros_like(cp), jnp.zeros_like(cp), core]).astype(jnp.int32)
        pieces = jnp.stack([cp, cp ^ 1, cp ^ 2, cp ^ 3]).astype(jnp.int32)

        w3 = (w_q, w_k, w_v)
        qkv = project(hidden, got[1], near, (0, rows), *w3, cos, sin, qkv_shape=(rows, 2, 2 * seq, width))

        sent = {}

        def send(row, o2, o3, o1):
            for s, o in ((2, o2), (3, o3), (1, o1)):
                sent[s, row] = lax.ppermute(o, "cp", swaps[s])

        def far_rows(qkv, row):
            return project(got[2], got[3], far, (row, 1), *w3, cos, sin, qkv=qkv)

        attn, peaks = None, []
        for row in range(rows):
            qkv = far_rows(qkv, row)
            attn, peak = attend(qkv, row, attn)
            peaks.append(peak[:, :width // peak.shape[0] // HEAD_DIM, 0].reshape(width // HEAD_DIM))
            pieces_of = attn.reshape(rows, cp_size, seq, width)
            if row < rows - 1:
                send(row, *out_far(pieces_of, w_o, pieces, row))
        n_heads = width // HEAD_DIM
        local = functools.reduce(jnp.maximum, peaks) * SCALE
        block = jnp.full((8, max(n_heads, 128)), -jnp.inf, F32).at[0, :n_heads].set(local)
        head_max = jnp.max(gather_small(block, (("dp", dp_size), ("cp", cp_size)), 1)[:, 0, :n_heads], axis=0)
        factor = jnp.where(head_max > TAU_CLIP, jnp.sqrt(TAU_CLIP / head_max), 1.0)
        col_factor = jnp.repeat(factor, HEAD_DIM)[None, :]
        *last, w_q_new = out_far(pieces_of, w_o, pieces, rows - 1, (w_q, col_factor))
        send(rows - 1, *last)
        out, w_k_new = out_own(pieces_of, w_o, pieces, batch, w_k, col_factor)
        for row in range(rows):
            for s in (1, 2, 3):
                out = lax.dynamic_update_slice(out, sent[s, row][None], ((cp ^ s) * rows + row, 0, 0))
        return out, head_max, w_q_new, w_k_new

    return jax.shard_map(
        compute,
        mesh=mesh,
        in_specs=(P("dp", "cp", None), P("cp"), P(None, None), P(None, None), P(None, None), P(None, None)),
        out_specs=(P("dp", "cp", None), P(None), P(None, None), P(None, None)),
        check_vma=False,
    )
```

```python
import functools

import jax
import jax.numpy as jnp
from jax import lax
from jax.experimental import pallas as pl
from jax.experimental.pallas import tpu as pltpu
from jax.sharding import PartitionSpec as P


HEAD_DIM = 128
TAU_CLIP = 100.0
ROPE_THETA = 50000.0
LOG2_E = 1.4426950408889634
SCALE = HEAD_DIM ** -0.5
MIB = 1024 * 1024
BF16 = jnp.bfloat16
F32 = jnp.float32
ANY = pl.BlockSpec(memory_space=pl.ANY)


def params(mib=60, **kw):
    return pltpu.CompilerParams(vmem_limit_bytes=mib * MIB, dimension_semantics=("arbitrary",), **kw)


def cost(flops, nbytes):
    return pl.CostEstimate(flops=int(flops), bytes_accessed=int(nbytes), transcendentals=0)


def gather_kernel(axes, src, out, send_sems, recv_sems):
    sizes = [n for _, n in axes]
    me = [lax.axis_index(a) for a, _ in axes]
    total = 1
    for n in sizes:
        total *= n
    my_slot = 0
    for i, n in zip(me, sizes):
        my_slot = my_slot * n + i
    shifts = []
    for lin in range(1, total):
        rest, sh = lin, []
        for n in reversed(sizes):
            sh.insert(0, rest % n)
            rest //= n
        shifts.append(sh)

    def peer(sh):
        return {a: lax.rem(i + d, n) for (a, n), i, d in zip(axes, me, sh)}

    barrier = pltpu.get_barrier_semaphore()
    for sh in shifts:
        pl.semaphore_signal(barrier, inc=1, device_id=peer(sh), device_id_type=pl.DeviceIdType.MESH)
    pl.semaphore_wait(barrier, total - 1)
    copies = []
    for j, sh in enumerate(shifts):
        copy = pltpu.make_async_remote_copy(
            src_ref=src, dst_ref=out.at[my_slot], send_sem=send_sems.at[j], recv_sem=recv_sems.at[j],
            device_id=peer(sh), device_id_type=pl.DeviceIdType.MESH)
        copy.start()
        copies.append(copy)
    out[my_slot] = src[...]
    for copy in copies:
        copy.wait()


def gather_small(x, axes, collective_id):
    total = 1
    for _, n in axes:
        total *= n
    return pl.pallas_call(
        functools.partial(gather_kernel, axes),
        out_shape=jax.ShapeDtypeStruct((total,) + x.shape, x.dtype),
        in_specs=[pl.BlockSpec(memory_space=pltpu.VMEM)],
        out_specs=pl.BlockSpec(memory_space=pltpu.VMEM),
        scratch_shapes=[pltpu.SemaphoreType.DMA((total - 1,)), pltpu.SemaphoreType.DMA((total - 1,))],
        compiler_params=pltpu.CompilerParams(collective_id=collective_id, has_side_effects=True),
        name="gather_small",
    )(x)


def rotate_into(t, cos_t, sin_t, out):
    for j in range(t.shape[1] // HEAD_DIM):
        h = t[:, j * HEAD_DIM:(j + 1) * HEAD_DIM]
        out[:, j * HEAD_DIM:(j + 1) * HEAD_DIM] = (h * cos_t + pltpu.roll(h, HEAD_DIM // 2, 1) * sin_t).astype(BF16)


def near_kernel(where, xa, xb, wq, wk, wv, cos, sin, q_out, k_out, v_out, xs, sems):
    nr, _, seq, dim = xs.shape

    @pl.when(pl.program_id(0) == 0)
    def _():
        ca = pltpu.make_async_copy(xa.at[pl.ds(where[1], nr)], xs.at[:, where[3]], sems.at[0])
        cb = pltpu.make_async_copy(xb, xs.at[:, 1 - where[3]], sems.at[1])
        ca.start()
        cb.start()
        ca.wait()
        cb.wait()

    half = 2 * seq
    x = xs[...].reshape(nr * half, dim)
    cos_t, sin_t = cos[...], sin[...]
    for w, out in ((wq, q_out), (wk, k_out)):
        t = jnp.dot(x, w[...], preferred_element_type=F32)
        for r in range(nr):
            rotate_into(t[r * half:(r + 1) * half], cos_t, sin_t, out.at[r])
    v_out[...] = jnp.dot(x, wv[...], preferred_element_type=F32).astype(BF16).reshape(nr, half, wv.shape[1])


def project_near(hidden, mate, where, w_q, w_k, w_v, cos, sin):
    dim, width = w_q.shape
    nr, seq, _ = mate.shape
    bn = min(256, width)
    half = 2 * seq
    tokens = nr * half
    w_spec = pl.BlockSpec((dim, bn), lambda n, w: (0, n))
    t_spec = pl.BlockSpec((half, HEAD_DIM), lambda n, w: (w[0], 0), pipeline_mode=pl.Buffered(buffer_count=1))
    return pl.pallas_call(
        near_kernel,
        grid_spec=pltpu.PrefetchScalarGridSpec(
            num_scalar_prefetch=1, grid=(width // bn,),
            in_specs=[ANY, ANY, w_spec, w_spec, w_spec, t_spec, t_spec],
            out_specs=[pl.BlockSpec((nr, half, bn), lambda n, w: (0, 0, n))] * 3,
            scratch_shapes=[pltpu.VMEM((nr, 2, seq, dim), BF16), pltpu.SemaphoreType.DMA((2,))]),
        out_shape=[jax.ShapeDtypeStruct((nr, half, width), BF16)] * 3,
        compiler_params=params(),
        cost_estimate=cost(6 * tokens * dim * width, 6 * dim * width + 2 * tokens * (dim + 3 * width)),
        name="project_near",
    )(where, hidden, mate, w_q, w_k, w_v, cos, sin)


def scores(kb, qb, s_ref, blk):
    for i in range(qb.shape[0] // blk):
        hi = (i + 1) * blk
        s_ref[i, :hi, :] = lax.dot_general(
            kb[:hi], qb[i * blk:hi], (((1,), (1,)), ((), ())), preferred_element_type=F32)


def soften(s_ref, p_ref, blk):
    keep = lax.broadcasted_iota(jnp.int32, (blk, blk), 0) <= lax.broadcasted_iota(jnp.int32, (blk, blk), 1)
    best, inverse = None, []
    for i in range(s_ref.shape[0]):
        lo, hi = i * blk, (i + 1) * blk
        diag = jnp.where(keep, s_ref[i, lo:hi, :], -jnp.inf)
        m = jnp.max(diag, axis=0, keepdims=True)
        if i:
            m = jnp.maximum(m, jnp.max(s_ref[i, :lo, :], axis=0, keepdims=True))
        best = m if best is None else jnp.maximum(best, m)
        p = jnp.exp2((diag - m) * (SCALE * LOG2_E))
        total = jnp.sum(p, axis=0, keepdims=True)
        p_ref[i, lo:hi, :] = p.astype(BF16)
        if i:
            p = jnp.exp2((s_ref[i, :lo, :] - m) * (SCALE * LOG2_E))
            total = total + jnp.sum(p, axis=0, keepdims=True)
            p_ref[i, :lo, :] = p.astype(BF16)
        inverse.append(1.0 / total)
    return best, inverse


def weigh(vb, p_ref, blk, inverse, out):
    for i in range(p_ref.shape[0]):
        lo, hi = i * blk, (i + 1) * blk
        o = lax.dot_general(vb[:hi], p_ref[i, :hi, :], (((0,), (0,)), ((), ())), preferred_element_type=F32)
        out[lo:hi, :] = (o * inverse[i]).T.astype(BF16)


def row_kernel(row, blk, where, xa, xb, wq, wk, wv, cos, sin, qn, kn, vn, *rest):
    out, peak, xs, qb, kb, vb, s_ref, p_ref, sems = rest[-9:]
    n = pl.program_id(0)
    last = pl.num_programs(0) - 1
    _, seq, dim = xs.shape
    half = 2 * seq
    heads = qb.shape[1] // HEAD_DIM
    cols = [slice(j * HEAD_DIM, (j + 1) * HEAD_DIM) for j in range(heads)]
    far0 = pl.multiple_of(where[0] * half, half)
    near0 = pl.multiple_of((1 - where[0]) * half, half)

    @pl.when(n == 0)
    def _():
        ca = pltpu.make_async_copy(xa.at[row], xs.at[where[3]], sems.at[0])
        cb = pltpu.make_async_copy(xb.at[row], xs.at[1 - where[3]], sems.at[1])
        ca.start()
        cb.start()
        ca.wait()
        cb.wait()

    def finish(j, soft):
        best, inverse = soft
        weigh(vb[:, cols[j]], p_ref.at[j], blk, inverse, out.at[0, :, cols[j]])
        peak[0, j:j + 1] = jnp.broadcast_to(jnp.max(best, axis=1, keepdims=True), (1, HEAD_DIM))

    @pl.when(n < last)
    def _():
        x = xs[...].reshape(half, dim)
        for j in range(heads):
            scores(kb[:, cols[j]], qb[:, cols[j]], s_ref.at[j], blk)
        rotate_into(jnp.dot(x, wq[...], preferred_element_type=F32), cos[...], sin[...], qb.at[pl.ds(far0, half)])
        soft = [soften(s_ref.at[j], p_ref.at[j], blk) for j in range(heads)]
        rotate_into(jnp.dot(x, wk[...], preferred_element_type=F32), cos[...], sin[...], kb.at[pl.ds(far0, half)])
        for j in range(heads):
            finish(j, soft[j])
        cut = half * 2 // 3
        vb[pl.ds(far0, cut)] = jnp.dot(x[:cut], wv[...], preferred_element_type=F32).astype(BF16)
        vb[pl.ds(far0 + cut, half - cut)] = jnp.dot(x[cut:], wv[...], preferred_element_type=F32).astype(BF16)
        qb[pl.ds(near0, half)] = qn[0]
        kb[pl.ds(near0, half)] = kn[0]
        vb[pl.ds(near0, half)] = vn[0]

    @pl.when(n == last)
    def _():
        for j in range(heads):
            scores(kb[:, cols[j]], qb[:, cols[j]], s_ref.at[j], blk)
        for j in range(heads):
            finish(j, soften(s_ref.at[j], p_ref.at[j], blk))


def row_attention(xa, xb, where, row, w_q, w_k, w_v, cos, sin, near, attn=None):
    dim, width = w_q.shape
    rows, seq, _ = xa.shape
    bn = min(256, width)
    blk = 256
    half = 2 * seq
    steps = width // bn
    now = lambda n: jnp.minimum(n, steps - 1)
    before = lambda n: jnp.maximum(n - 1, 0)
    w_spec = pl.BlockSpec((dim, bn), lambda n, w: (0, now(n)))
    t_spec = pl.BlockSpec((half, HEAD_DIM), lambda n, w: (w[0], 0), pipeline_mode=pl.Buffered(buffer_count=1))
    n_spec = pl.BlockSpec((1, half, bn), lambda n, w: (row, 0, now(n)))
    old = [] if attn is None else [attn]
    heads = bn // HEAD_DIM
    n_blk = 2 * half // blk
    return pl.pallas_call(
        functools.partial(row_kernel, row, blk),
        grid_spec=pltpu.PrefetchScalarGridSpec(
            num_scalar_prefetch=1, grid=(steps + 1,),
            in_specs=[ANY, ANY, w_spec, w_spec, w_spec, t_spec, t_spec, n_spec, n_spec, n_spec] + [ANY] * len(old),
            out_specs=[pl.BlockSpec((1, 2 * half, bn), lambda n, w: (row, 0, before(n))),
                       pl.BlockSpec((1, 8, HEAD_DIM), lambda n, w: (before(n), 0, 0))],
            scratch_shapes=[
                pltpu.VMEM((2, seq, dim), BF16), *[pltpu.VMEM((2 * half, bn), BF16)] * 3,
                pltpu.VMEM((heads, n_blk, 2 * half, blk), F32), pltpu.VMEM((heads, n_blk, 2 * half, blk), BF16),
                pltpu.SemaphoreType.DMA((2,))]),
        out_shape=[jax.ShapeDtypeStruct((rows, 2 * half, width), BF16), jax.ShapeDtypeStruct((steps, 8, HEAD_DIM), F32)],
        input_output_aliases={11: 0} if old else {},
        compiler_params=params(),
        cost_estimate=cost(6 * half * dim * width + 16 * half * half * width, 6 * dim * width),
        name="row_attention",
    )(where, xa, xb, w_q, w_k, w_v, cos, sin, *near, *old)


def load_tokens(pieces, attn, xs, sems):
    copies = [pltpu.make_async_copy(attn.at[r, p], xs.at[i], sems.at[i]) for i, (r, p) in enumerate(pieces)]
    for c in copies:
        c.start()
    for c in copies:
        c.wait()


def clip_into(w_in, factor, w_new):
    for h in range(w_in.shape[1] // HEAD_DIM):
        c = slice(h * HEAD_DIM, (h + 1) * HEAD_DIM)
        w_new[:, c] = (w_in[:, c].astype(F32) * factor[:, c]).astype(BF16)


def out_far_kernel(row, clip, where, attn, w_o, *rest):
    if clip:
        w_in, factor, o2, o3, o1, w_new, xs, sems = rest
    else:
        o2, o3, o1, xs, sems = rest

    @pl.when(pl.program_id(0) == 0)
    def _():
        load_tokens([(row, where[2]), (row, where[3]), (row, where[1])], attn, xs, sems)

    n_pieces, seq, width = xs.shape
    y = jnp.dot(xs[...].reshape(n_pieces * seq, width), w_o[...], preferred_element_type=F32).astype(BF16)
    o2[...] = y[:seq]
    o3[...] = y[seq:2 * seq]
    o1[...] = y[2 * seq:]
    if clip:
        clip_into(w_in, factor, w_new)


def out_far(attn, w_o, where, row, clip=None):
    _, _, seq, width = attn.shape
    dim = w_o.shape[1]
    bn = min(512, dim) if clip is None else min(256, dim)
    steps = dim // bn
    o_spec = pl.BlockSpec((seq, bn), lambda n, w: (0, n))
    in_specs = [ANY, pl.BlockSpec((width, bn), lambda n, w: (0, n))]
    out_specs = [o_spec] * 3
    out_shape = [jax.ShapeDtypeStruct((seq, dim), BF16)] * 3
    args = [attn, w_o]
    if clip is not None:
        w_in, factor = clip
        c_spec = pl.BlockSpec((w_in.shape[0] // steps, width), lambda n, w: (n, 0))
        in_specs += [c_spec, pl.BlockSpec((1, width), lambda n, w: (0, 0))]
        out_specs = out_specs + [c_spec]
        out_shape = out_shape + [jax.ShapeDtypeStruct(w_in.shape, BF16)]
        args += [w_in, factor]
    return pl.pallas_call(
        functools.partial(out_far_kernel, row, clip is not None),
        grid_spec=pltpu.PrefetchScalarGridSpec(
            num_scalar_prefetch=1, grid=(steps,), in_specs=in_specs, out_specs=out_specs,
            scratch_shapes=[pltpu.VMEM((3, seq, width), BF16), pltpu.SemaphoreType.DMA((3,))]),
        out_shape=out_shape,
        compiler_params=params(),
        cost_estimate=cost(6 * seq * dim * width, 2 * dim * width + 6 * seq * (dim + width)),
        name="out_far",
    )(where, *args)


def out_own_kernel(n_got, where, attn, w_o, w_in, factor, *rest):
    got, (out, w_new, xs, sems) = rest[:-4], rest[-4:]

    @pl.when(pl.program_id(0) == 0)
    def _():
        load_tokens([(r, where[0]) for r in range(xs.shape[0])], attn, xs, sems)

    n_pieces, seq, width = xs.shape
    for i, piece in enumerate(got):
        out[where[1 + i // n_got], i % n_got] = piece[...]
    y = jnp.dot(xs[...].reshape(n_pieces * seq, width), w_o[...], preferred_element_type=F32).astype(BF16)
    out[where[0]] = y.reshape(n_pieces, seq, y.shape[1])
    clip_into(w_in, factor, w_new)


def out_own(attn, w_o, where, w_in, factor, got):
    rows, n_pieces, seq, width = attn.shape
    dim = w_o.shape[1]
    bn = min(256, dim)
    steps = dim // bn
    c_spec = pl.BlockSpec((w_in.shape[0] // steps, width), lambda n, w: (n, 0))
    g_spec = pl.BlockSpec((seq, bn), lambda n, w: (0, n))
    flat = [g for gs in got for g in gs]
    return pl.pallas_call(
        functools.partial(out_own_kernel, len(got[0])),
        grid_spec=pltpu.PrefetchScalarGridSpec(
            num_scalar_prefetch=1, grid=(steps,),
            in_specs=[ANY, pl.BlockSpec((width, bn), lambda n, w: (0, n)), c_spec,
                      pl.BlockSpec((1, width), lambda n, w: (0, 0))] + [g_spec] * len(flat),
            out_specs=[pl.BlockSpec((n_pieces, rows, seq, bn), lambda n, w: (0, 0, 0, n)), c_spec],
            scratch_shapes=[pltpu.VMEM((rows, seq, width), BF16), pltpu.SemaphoreType.DMA((rows,))]),
        out_shape=[jax.ShapeDtypeStruct((n_pieces, rows, seq, dim), BF16), jax.ShapeDtypeStruct(w_in.shape, BF16)],
        compiler_params=params(),
        cost_estimate=cost(2 * rows * seq * dim * width, 6 * dim * width),
        name="out_own",
    )(where, attn, w_o, w_in, factor, *flat)


def rope_tables(pos_ids):
    half_dim = HEAD_DIM // 2
    inv_freq = jnp.float32(ROPE_THETA) ** (-jnp.arange(half_dim, dtype=F32) * (2.0 / HEAD_DIM))
    angle = pos_ids.astype(F32)[:, None] * inv_freq[None, :]
    cos_t, sin_t = jnp.cos(angle), jnp.sin(angle)
    return jnp.concatenate([cos_t, cos_t], axis=1), jnp.concatenate([-sin_t, sin_t], axis=1)


def solution(mesh):
    cp_size = mesh.shape["cp"]
    dp_size = mesh.shape["dp"]
    assert cp_size == 4
    swaps = {s: [(i, i ^ s) for i in range(cp_size)] for s in (1, 2, 3)}

    def compute(hidden, pos_ids, w_q, w_k, w_v, w_o):
        batch, seq, _ = hidden.shape
        width = w_q.shape[1]
        rows = batch // cp_size
        n_heads = width // HEAD_DIM
        cp = lax.axis_index("cp").astype(jnp.int32)
        chip, core = cp // 2, cp % 2

        pos_block = jnp.zeros((8, 256), jnp.int32).at[0, :seq].set(pos_ids)
        all_pos = gather_small(pos_block, (("cp", cp_size),), 0)[:, 0, :seq].reshape(cp_size * seq)

        def outgoing(s, cp):
            return lax.dynamic_slice_in_dim(hidden, (cp ^ s) * rows, rows, axis=0)

        got = {}
        first, after = lax.optimization_barrier((cp, all_pos))
        piece = outgoing(1, first)
        got[1] = lax.ppermute(piece, "cp", swaps[1])
        second, _ = lax.optimization_barrier((cp, piece))
        for s in (2, 3):
            got[s] = lax.ppermute(outgoing(s, second), "cp", swaps[s])

        cos, sin = rope_tables(after)
        zero = jnp.zeros_like(cp)
        near_at = jnp.stack([chip, cp * rows, zero, core]).astype(jnp.int32)
        far_at = jnp.stack([1 - chip, zero, zero, core]).astype(jnp.int32)
        pieces = jnp.stack([cp, cp ^ 1, cp ^ 2, cp ^ 3]).astype(jnp.int32)

        w3 = (w_q, w_k, w_v)
        near = project_near(hidden, got[1], near_at, *w3, cos, sin)

        sent = {}

        def send(row, o2, o3, o1):
            for s, o in ((2, o2), (3, o3), (1, o1)):
                sent[s, row] = lax.ppermute(o, "cp", swaps[s])

        attn, peaks = None, []
        for row in range(rows):
            attn, peak = row_attention(got[2], got[3], far_at, row, *w3, cos, sin, near, attn)
            peaks.append(peak[:, :n_heads // peak.shape[0], 0].reshape(n_heads))
            pieces_of = attn.reshape(rows, cp_size, seq, width)
            if row < rows - 1:
                send(row, *out_far(pieces_of, w_o, pieces, row))
        local = functools.reduce(jnp.maximum, peaks) * SCALE
        block = jnp.full((8, max(n_heads, 128)), -jnp.inf, F32).at[0, :n_heads].set(local)
        head_max = jnp.max(gather_small(block, (("dp", dp_size), ("cp", cp_size)), 1)[:, 0, :n_heads], axis=0)
        factor = jnp.where(head_max > TAU_CLIP, jnp.sqrt(TAU_CLIP / head_max), 1.0)
        col_factor = jnp.repeat(factor, HEAD_DIM)[None, :]
        *last, w_q_new = out_far(pieces_of, w_o, pieces, rows - 1, (w_q, col_factor))
        send(rows - 1, *last)
        out, w_k_new = out_own(
            pieces_of, w_o, pieces, w_k, col_factor, [[sent[s, r] for r in range(rows - 1)] for s in (1, 2, 3)])
        for s in (1, 2, 3):
            out = lax.dynamic_update_slice(out, sent[s, rows - 1][None, None], (cp ^ s, rows - 1, 0, 0))
        return out.reshape(hidden.shape), head_max, w_q_new, w_k_new

    return jax.shard_map(
        compute,
        mesh=mesh,
        in_specs=(P("dp", "cp", None), P("cp"), P(None, None), P(None, None), P(None, None), P(None, None)),
        out_specs=(P("dp", "cp", None), P(None), P(None, None), P(None, None)),
        check_vma=False,
    )
```

```python
import functools

import jax
import jax.numpy as jnp
from jax import lax
from jax.experimental import pallas as pl
from jax.experimental.pallas import tpu as pltpu
from jax.sharding import PartitionSpec as P


HEAD_DIM = 128
TAU_CLIP = 100.0
ROPE_THETA = 50000.0
LOG2_E = 1.4426950408889634
SCALE = HEAD_DIM ** -0.5
MIB = 1024 * 1024
BF16 = jnp.bfloat16
F32 = jnp.float32
ANY = pl.BlockSpec(memory_space=pl.ANY)


def params(mib=60, **kw):
    return pltpu.CompilerParams(vmem_limit_bytes=mib * MIB, dimension_semantics=("arbitrary",), **kw)


def cost(flops, nbytes):
    return pl.CostEstimate(flops=int(flops), bytes_accessed=int(nbytes), transcendentals=0)


def gather_kernel(axes, src, out, send_sems, recv_sems):
    sizes = [n for _, n in axes]
    me = [lax.axis_index(a) for a, _ in axes]
    total = 1
    for n in sizes:
        total *= n
    my_slot = 0
    for i, n in zip(me, sizes):
        my_slot = my_slot * n + i
    shifts = []
    for lin in range(1, total):
        rest, sh = lin, []
        for n in reversed(sizes):
            sh.insert(0, rest % n)
            rest //= n
        shifts.append(sh)

    def peer(sh):
        return {a: lax.rem(i + d, n) for (a, n), i, d in zip(axes, me, sh)}

    barrier = pltpu.get_barrier_semaphore()
    for sh in shifts:
        pl.semaphore_signal(barrier, inc=1, device_id=peer(sh), device_id_type=pl.DeviceIdType.MESH)
    pl.semaphore_wait(barrier, total - 1)
    copies = []
    for j, sh in enumerate(shifts):
        copy = pltpu.make_async_remote_copy(
            src_ref=src, dst_ref=out.at[my_slot], send_sem=send_sems.at[j], recv_sem=recv_sems.at[j],
            device_id=peer(sh), device_id_type=pl.DeviceIdType.MESH)
        copy.start()
        copies.append(copy)
    out[my_slot] = src[...]
    for copy in copies:
        copy.wait()


def gather_small(x, axes, collective_id):
    total = 1
    for _, n in axes:
        total *= n
    return pl.pallas_call(
        functools.partial(gather_kernel, axes),
        out_shape=jax.ShapeDtypeStruct((total,) + x.shape, x.dtype),
        in_specs=[pl.BlockSpec(memory_space=pltpu.VMEM)],
        out_specs=pl.BlockSpec(memory_space=pltpu.VMEM),
        scratch_shapes=[pltpu.SemaphoreType.DMA((total - 1,)), pltpu.SemaphoreType.DMA((total - 1,))],
        compiler_params=pltpu.CompilerParams(collective_id=collective_id, has_side_effects=True),
        name="gather_small",
    )(x)


def rotate_into(t, cos_t, sin_t, out):
    for j in range(t.shape[1] // HEAD_DIM):
        h = t[:, j * HEAD_DIM:(j + 1) * HEAD_DIM]
        out[:, j * HEAD_DIM:(j + 1) * HEAD_DIM] = (h * cos_t + pltpu.roll(h, HEAD_DIM // 2, 1) * sin_t).astype(BF16)


def near_kernel(where, xa, xb, wq, wk, wv, cos, sin, q_out, k_out, v_out, xs, sems):
    nr, _, seq, dim = xs.shape

    @pl.when(pl.program_id(0) == 0)
    def _():
        ca = pltpu.make_async_copy(xa.at[pl.ds(where[1], nr)], xs.at[:, where[3]], sems.at[0])
        cb = pltpu.make_async_copy(xb, xs.at[:, 1 - where[3]], sems.at[1])
        ca.start()
        cb.start()
        ca.wait()
        cb.wait()

    half = 2 * seq
    x = xs[...].reshape(nr * half, dim)
    cos_t, sin_t = cos[...], sin[...]
    for w, out in ((wq, q_out), (wk, k_out)):
        t = jnp.dot(x, w[...], preferred_element_type=F32)
        for r in range(nr):
            rotate_into(t[r * half:(r + 1) * half], cos_t, sin_t, out.at[r])
    v_out[...] = jnp.dot(x, wv[...], preferred_element_type=F32).astype(BF16).reshape(nr, half, wv.shape[1])


def project_near(hidden, mate, where, w_q, w_k, w_v, cos, sin):
    dim, width = w_q.shape
    nr, seq, _ = mate.shape
    bn = min(256, width)
    half = 2 * seq
    tokens = nr * half
    w_spec = pl.BlockSpec((dim, bn), lambda n, w: (0, n))
    t_spec = pl.BlockSpec((half, HEAD_DIM), lambda n, w: (w[0], 0), pipeline_mode=pl.Buffered(buffer_count=1))
    return pl.pallas_call(
        near_kernel,
        grid_spec=pltpu.PrefetchScalarGridSpec(
            num_scalar_prefetch=1, grid=(width // bn,),
            in_specs=[ANY, ANY, w_spec, w_spec, w_spec, t_spec, t_spec],
            out_specs=[pl.BlockSpec((nr, half, bn), lambda n, w: (0, 0, n))] * 3,
            scratch_shapes=[pltpu.VMEM((nr, 2, seq, dim), BF16), pltpu.SemaphoreType.DMA((2,))]),
        out_shape=[jax.ShapeDtypeStruct((nr, half, width), BF16)] * 3,
        compiler_params=params(),
        cost_estimate=cost(6 * tokens * dim * width, 6 * dim * width + 2 * tokens * (dim + 3 * width)),
        name="project_near",
    )(where, hidden, mate, w_q, w_k, w_v, cos, sin)


def scores(kb, qb, s_ref, blk):
    for i in range(qb.shape[0] // blk):
        hi = (i + 1) * blk
        s_ref[i, :hi, :] = lax.dot_general(
            kb[:hi], qb[i * blk:hi], (((1,), (1,)), ((), ())), preferred_element_type=F32)


def soften(s_ref, p_ref, blk):
    keep = lax.broadcasted_iota(jnp.int32, (blk, blk), 0) <= lax.broadcasted_iota(jnp.int32, (blk, blk), 1)
    best, inverse = None, []
    for i in range(s_ref.shape[0]):
        lo, hi = i * blk, (i + 1) * blk
        diag = jnp.where(keep, s_ref[i, lo:hi, :], -jnp.inf)
        m = jnp.max(diag, axis=0, keepdims=True)
        if i:
            m = jnp.maximum(m, jnp.max(s_ref[i, :lo, :], axis=0, keepdims=True))
        best = m if best is None else jnp.maximum(best, m)
        p = jnp.exp2((diag - m) * (SCALE * LOG2_E))
        total = jnp.sum(p, axis=0, keepdims=True)
        p_ref[i, lo:hi, :] = p.astype(BF16)
        if i:
            p = jnp.exp2((s_ref[i, :lo, :] - m) * (SCALE * LOG2_E))
            total = total + jnp.sum(p, axis=0, keepdims=True)
            p_ref[i, :lo, :] = p.astype(BF16)
        inverse.append(1.0 / total)
    return best, inverse


def weigh(vb, p_ref, blk, inverse, out):
    for i in range(p_ref.shape[0]):
        lo, hi = i * blk, (i + 1) * blk
        o = lax.dot_general(vb[:hi], p_ref[i, :hi, :], (((0,), (0,)), ((), ())), preferred_element_type=F32)
        out[lo:hi, :] = (o * inverse[i]).T.astype(BF16)


def rows_kernel(r0, nr, blk, copies, where, xa, xb, wq, wk, wv, cos, sin, qn, kn, vn, *rest):
    if copies:
        out, peak, wq_copy, wk_copy, xs, qb, kb, vb, s_ref, p_ref, sems, copy_sems = rest[-12:]
    else:
        out, peak, xs, qb, kb, vb, s_ref, p_ref, sems = rest[-9:]
    t = pl.program_id(0)
    last = pl.num_programs(0) - 1
    r = lax.rem(t, nr)
    _, _, seq, dim = xs.shape
    half = 2 * seq
    bn = qb.shape[1]
    heads = bn // HEAD_DIM
    cols = [slice(j * HEAD_DIM, (j + 1) * HEAD_DIM) for j in range(heads)]
    far0 = pl.multiple_of(where[0] * half, half)
    near0 = pl.multiple_of((1 - where[0]) * half, half)

    def weight_copies():
        c = pl.ds(pl.multiple_of(lax.div(t, nr) * bn, bn), bn)
        return [pltpu.make_async_copy(w, o.at[:, c], copy_sems.at[i])
                for i, (w, o) in enumerate(((wq, wq_copy), (wk, wk_copy)))]

    @pl.when(t == 0)
    def _():
        ca = pltpu.make_async_copy(xa.at[pl.ds(r0, nr)], xs.at[:, where[3]], sems.at[0])
        cb = pltpu.make_async_copy(xb.at[pl.ds(r0, nr)], xs.at[:, 1 - where[3]], sems.at[1])
        ca.start()
        cb.start()
        ca.wait()
        cb.wait()

    if copies:
        @pl.when(jnp.logical_and(t < last, r == 0))
        def _():
            for c in weight_copies():
                c.start()

    def finish(j, soft):
        best, inverse = soft
        weigh(vb[:, cols[j]], p_ref.at[j], blk, inverse, out.at[0, :, cols[j]])
        peak[0, j:j + 1] = jnp.broadcast_to(jnp.max(best, axis=1, keepdims=True), (1, HEAD_DIM))

    @pl.when(t < last)
    def _():
        x = xs[r].reshape(half, dim)
        for j in range(heads):
            scores(kb[:, cols[j]], qb[:, cols[j]], s_ref.at[j], blk)
        rotate_into(jnp.dot(x, wq[...], preferred_element_type=F32), cos[...], sin[...], qb.at[pl.ds(far0, half)])
        soft = [soften(s_ref.at[j], p_ref.at[j], blk) for j in range(heads)]
        rotate_into(jnp.dot(x, wk[...], preferred_element_type=F32), cos[...], sin[...], kb.at[pl.ds(far0, half)])
        for j in range(heads):
            finish(j, soft[j])
        cut = half * 2 // 3
        vb[pl.ds(far0, cut)] = jnp.dot(x[:cut], wv[...], preferred_element_type=F32).astype(BF16)
        vb[pl.ds(far0 + cut, half - cut)] = jnp.dot(x[cut:], wv[...], preferred_element_type=F32).astype(BF16)
        qb[pl.ds(near0, half)] = qn[0]
        kb[pl.ds(near0, half)] = kn[0]
        vb[pl.ds(near0, half)] = vn[0]

    @pl.when(t == last)
    def _():
        for j in range(heads):
            scores(kb[:, cols[j]], qb[:, cols[j]], s_ref.at[j], blk)
        for j in range(heads):
            finish(j, soften(s_ref.at[j], p_ref.at[j], blk))

    if copies:
        @pl.when(jnp.logical_and(t < last, r == nr - 1))
        def _():
            for c in weight_copies():
                c.wait()


def rows_attention(xa, xb, where, r0, nr, w_q, w_k, w_v, cos, sin, near, attn=None, copies=False):
    dim, width = w_q.shape
    rows, seq, _ = xa.shape
    bn = min(256, width)
    blk = 256
    half = 2 * seq
    total = width // bn * nr
    now = lambda t: jnp.minimum(t, total - 1)
    before = lambda t: jnp.maximum(t - 1, 0)
    w_spec = pl.BlockSpec((dim, bn), lambda t, w: (0, now(t) // nr))
    t_spec = pl.BlockSpec((half, HEAD_DIM), lambda t, w: (w[0], 0), pipeline_mode=pl.Buffered(buffer_count=1))
    n_spec = pl.BlockSpec((1, half, bn), lambda t, w: (r0 + now(t) % nr, 0, now(t) // nr))
    old = [] if attn is None else [attn]
    heads = bn // HEAD_DIM
    n_blk = 2 * half // blk
    more_shapes = [jax.ShapeDtypeStruct((dim, width), BF16)] * 2 if copies else []
    return pl.pallas_call(
        functools.partial(rows_kernel, r0, nr, blk, copies),
        grid_spec=pltpu.PrefetchScalarGridSpec(
            num_scalar_prefetch=1, grid=(total + 1,),
            in_specs=[ANY, ANY, w_spec, w_spec, w_spec, t_spec, t_spec, n_spec, n_spec, n_spec] + [ANY] * len(old),
            out_specs=[pl.BlockSpec((1, 2 * half, bn), lambda t, w: (r0 + before(t) % nr, 0, before(t) // nr)),
                       pl.BlockSpec((1, 8, HEAD_DIM), lambda t, w: (before(t), 0, 0))] + [ANY] * len(more_shapes),
            scratch_shapes=[
                pltpu.VMEM((nr, 2, seq, dim), BF16), *[pltpu.VMEM((2 * half, bn), BF16)] * 3,
                pltpu.VMEM((heads, n_blk, 2 * half, blk), F32), pltpu.VMEM((heads, n_blk, 2 * half, blk), BF16),
                pltpu.SemaphoreType.DMA((2,))] + ([pltpu.SemaphoreType.DMA((2,))] if copies else [])),
        out_shape=[jax.ShapeDtypeStruct((rows, 2 * half, width), BF16), jax.ShapeDtypeStruct((total, 8, HEAD_DIM), F32)]
        + more_shapes,
        input_output_aliases={11: 0} if old else {},
        compiler_params=params(),
        cost_estimate=cost(nr * (6 * half * dim * width + 16 * half * half * width), (10 if copies else 6) * dim * width),
        name="rows_attention",
    )(where, xa, xb, w_q, w_k, w_v, cos, sin, *near, *old)


def load_tokens(pieces, attn, xs, sems):
    copies = [pltpu.make_async_copy(attn.at[r, p], xs.at[i], sems.at[i]) for i, (r, p) in enumerate(pieces)]
    for c in copies:
        c.start()
    for c in copies:
        c.wait()


class Clip:
    def __init__(self, factor, w, order, ring, in_sems, out_sems):
        self.factor, self.w, self.order, self.ring, self.in_sems, self.out_sems = factor, w, order, ring, in_sems, out_sems
        self.slots = ring.shape[0]
        self.n = pl.program_id(0)
        self.steps = pl.num_programs(0)

    @staticmethod
    def scratch(dim, n_heads, steps):
        slots = 2 * -(-n_heads // steps)
        return [pltpu.SMEM((n_heads + 1,), jnp.int32), pltpu.VMEM((slots, dim, HEAD_DIM), BF16),
                pltpu.SemaphoreType.DMA((slots,)), pltpu.SemaphoreType.DMA((slots,))]

    def columns(self, i):
        return self.w.at[:, pl.ds(pl.multiple_of(self.order[i] * HEAD_DIM, HEAD_DIM), HEAD_DIM)]

    def fetch(self, i):
        s = lax.rem(i, self.slots)
        return pltpu.make_async_copy(self.columns(i), self.ring.at[s], self.in_sems.at[s])

    def put(self, i):
        s = lax.rem(i, self.slots)
        return pltpu.make_async_copy(self.ring.at[s], self.columns(i), self.out_sems.at[s])

    def share(self, n):
        count = self.order[self.order.shape[0] - 1]
        return lax.div(n * count, self.steps), lax.div((n + 1) * count, self.steps)

    def ahead(self):
        n_heads = self.order.shape[0] - 1

        @pl.when(self.n == 0)
        def _():
            self.order[n_heads] = 0

            @pl.loop(0, n_heads)
            def _(h):
                @pl.when(self.factor[h] < 1.0)
                def _():
                    k = self.order[n_heads]
                    self.order[k] = h
                    self.order[n_heads] = k + 1

            @pl.loop(*self.share(0))
            def _(i):
                self.fetch(i).start()

        @pl.when(self.n + 1 < self.steps)
        def _():
            @pl.loop(*self.share(self.n + 1))
            def _(i):
                @pl.when(i >= self.slots)
                def _():
                    self.put(i - self.slots).wait()

                self.fetch(i).start()

    def work(self):
        rows = self.ring.shape[1]
        part = rows // 4 if rows % 64 == 0 else rows

        @pl.loop(*self.share(self.n))
        def _(i):
            s = lax.rem(i, self.slots)
            self.fetch(i).wait()
            f = self.factor[self.order[i]]
            for lo in range(0, rows, part):
                self.ring[s, lo:lo + part] = (self.ring[s, lo:lo + part].astype(F32) * f).astype(BF16)
            self.put(i).start()

        @pl.when(self.n == self.steps - 1)
        def _():
            count = self.order[self.order.shape[0] - 1]

            @pl.loop(jnp.maximum(count - self.slots, 0), count)
            def _(i):
                self.put(i).wait()


def out_far_kernel(rows, clip, where, *refs):
    if clip:
        factor, attn, w_o, _, o2, o3, o1, w_new, xs, sems, *scratch = refs
        scaling = Clip(factor, w_new, *scratch)
    else:
        attn, w_o, o2, o3, o1, xs, sems = refs

    @pl.when(pl.program_id(0) == 0)
    def _():
        load_tokens([(r, where[i]) for i in (2, 3, 1) for r in rows], attn, xs, sems)

    if clip:
        scaling.ahead()
    n_pieces, seq, width = xs.shape
    y = jnp.dot(xs[...].reshape(n_pieces * seq, width), w_o[...], preferred_element_type=F32).astype(BF16)
    y = y.reshape(3, len(rows), seq, y.shape[1])
    o2[...] = y[0]
    o3[...] = y[1]
    o1[...] = y[2]
    if clip:
        scaling.work()


def out_far(attn, w_o, where, rows, clip=None):
    _, _, seq, width = attn.shape
    dim = w_o.shape[1]
    bn = min(512 if clip is None else 256, dim)
    steps = dim // bn
    nr = len(rows)
    prefetch, args = [where], [attn, w_o]
    in_specs = [ANY, pl.BlockSpec((width, bn), lambda n, *_: (0, n))]
    out_specs = [pl.BlockSpec((nr, seq, bn), lambda n, *_: (0, 0, n))] * 3
    out_shape = [jax.ShapeDtypeStruct((nr, seq, dim), BF16)] * 3
    scratch = [pltpu.VMEM((3 * nr, seq, width), BF16), pltpu.SemaphoreType.DMA((3 * nr,))]
    aliases = {}
    if clip is not None:
        factor, w_in = clip
        prefetch.append(factor)
        args.append(w_in)
        in_specs.append(ANY)
        out_specs.append(ANY)
        out_shape.append(jax.ShapeDtypeStruct(w_in.shape, BF16))
        scratch += Clip.scratch(w_in.shape[0], factor.shape[0], steps)
        aliases = {4: 3}
    return pl.pallas_call(
        functools.partial(out_far_kernel, rows, clip is not None),
        grid_spec=pltpu.PrefetchScalarGridSpec(
            num_scalar_prefetch=len(prefetch), grid=(steps,), in_specs=in_specs, out_specs=out_specs, scratch_shapes=scratch),
        out_shape=out_shape,
        input_output_aliases=aliases,
        compiler_params=params(),
        cost_estimate=cost(6 * nr * seq * dim * width, 2 * dim * width + 6 * nr * seq * (dim + width)),
        name="out_far",
    )(*prefetch, *args)


def out_own_kernel(n_got, where, factor, attn, w_o, _, *refs):
    got, (out, w_new, xs, sems, *scratch) = refs[:3 * n_got], refs[3 * n_got:]
    scaling = Clip(factor, w_new, *scratch)

    @pl.when(pl.program_id(0) == 0)
    def _():
        load_tokens([(r, where[0]) for r in range(xs.shape[0])], attn, xs, sems)

    scaling.ahead()
    n_pieces, seq, width = xs.shape
    for i, g in enumerate(got):
        out[where[1 + i // n_got], i % n_got] = g[0]
    y = jnp.dot(xs[...].reshape(n_pieces * seq, width), w_o[...], preferred_element_type=F32).astype(BF16)
    out[where[0]] = y.reshape(n_pieces, seq, y.shape[1])
    scaling.work()


def out_own(attn, w_o, where, factor, w_in, got):
    rows, n_pieces, seq, width = attn.shape
    dim = w_o.shape[1]
    bn = min(256, dim)
    steps = dim // bn
    g_spec = pl.BlockSpec((1, seq, bn), lambda n, *_: (0, 0, n))
    flat = [g for gs in got for g in gs]
    return pl.pallas_call(
        functools.partial(out_own_kernel, len(got[0])),
        grid_spec=pltpu.PrefetchScalarGridSpec(
            num_scalar_prefetch=2, grid=(steps,),
            in_specs=[ANY, pl.BlockSpec((width, bn), lambda n, *_: (0, n)), ANY] + [g_spec] * len(flat),
            out_specs=[pl.BlockSpec((n_pieces, rows, seq, bn), lambda n, *_: (0, 0, 0, n)), ANY],
            scratch_shapes=[pltpu.VMEM((rows, seq, width), BF16), pltpu.SemaphoreType.DMA((rows,))]
            + Clip.scratch(w_in.shape[0], factor.shape[0], steps)),
        out_shape=[jax.ShapeDtypeStruct((n_pieces, rows, seq, dim), BF16), jax.ShapeDtypeStruct(w_in.shape, BF16)],
        input_output_aliases={4: 1},
        compiler_params=params(),
        cost_estimate=cost(2 * rows * seq * dim * width, 6 * dim * width),
        name="out_own",
    )(where, factor, attn, w_o, w_in, *flat)


def rope_tables(pos_ids):
    half_dim = HEAD_DIM // 2
    inv_freq = jnp.float32(ROPE_THETA) ** (-jnp.arange(half_dim, dtype=F32) * (2.0 / HEAD_DIM))
    angle = pos_ids.astype(F32)[:, None] * inv_freq[None, :]
    cos_t, sin_t = jnp.cos(angle), jnp.sin(angle)
    return jnp.concatenate([cos_t, cos_t], axis=1), jnp.concatenate([-sin_t, sin_t], axis=1)


def solution(mesh):
    cp_size = mesh.shape["cp"]
    dp_size = mesh.shape["dp"]
    assert cp_size == 4
    swaps = {s: [(i, i ^ s) for i in range(cp_size)] for s in (1, 2, 3)}

    def compute(hidden, pos_ids, w_q, w_k, w_v, w_o):
        batch, seq, _ = hidden.shape
        width = w_q.shape[1]
        rows = batch // cp_size
        n_heads = width // HEAD_DIM
        cp = lax.axis_index("cp").astype(jnp.int32)
        chip, core = cp // 2, cp % 2

        pos_block = jnp.zeros((8, 256), jnp.int32).at[0, :seq].set(pos_ids)
        all_pos = gather_small(pos_block, (("cp", cp_size),), 0)[:, 0, :seq].reshape(cp_size * seq)

        def outgoing(s, cp):
            return lax.dynamic_slice_in_dim(hidden, (cp ^ s) * rows, rows, axis=0)

        got = {}
        first, after = lax.optimization_barrier((cp, all_pos))
        piece = outgoing(1, first)
        got[1] = lax.ppermute(piece, "cp", swaps[1])
        second, _ = lax.optimization_barrier((cp, piece))
        for s in (2, 3):
            got[s] = lax.ppermute(outgoing(s, second), "cp", swaps[s])

        cos, sin = rope_tables(after)
        zero = jnp.zeros_like(cp)
        near_at = jnp.stack([chip, cp * rows, zero, core]).astype(jnp.int32)
        far_at = jnp.stack([1 - chip, zero, zero, core]).astype(jnp.int32)
        pieces = jnp.stack([cp, cp ^ 1, cp ^ 2, cp ^ 3]).astype(jnp.int32)

        w3 = (w_q, w_k, w_v)
        near = project_near(hidden, got[1], near_at, *w3, cos, sin)

        def send(*outs):
            sent = {}
            for s, o in zip((2, 3, 1), outs):
                sent[s] = lax.ppermute(o, "cp", swaps[s])
            return sent

        def highest(peak):
            return jnp.max(peak[:, :per_step, 0].reshape(n_heads // per_step, -1, per_step), axis=1).reshape(n_heads)

        per_step = min(256, width) // HEAD_DIM
        attn, peak, w_q_copy, w_k_copy = rows_attention(
            got[2], got[3], far_at, 0, rows - 1, *w3, cos, sin, near, copies=True)
        pieces_of = attn.reshape(rows, cp_size, seq, width)
        early = []
        for row in range(rows - 1):
            outs = out_far(pieces_of, w_o, pieces, [row])
            early.append(send(*outs))
        attn, peak_last = rows_attention(got[2], got[3], far_at, rows - 1, 1, *w3, cos, sin, near, attn)
        pieces_of = attn.reshape(rows, cp_size, seq, width)
        local = jnp.maximum(highest(peak), highest(peak_last)) * SCALE
        block = jnp.full((8, max(n_heads, 128)), -jnp.inf, F32).at[0, :n_heads].set(local)
        head_max = jnp.max(gather_small(block, (("dp", dp_size), ("cp", cp_size)), 1)[:, 0, :n_heads], axis=0)
        factor = jnp.where(head_max > TAU_CLIP, jnp.sqrt(TAU_CLIP / head_max), 1.0)
        *outs, w_q_new = out_far(pieces_of, w_o, pieces, [rows - 1], (factor, w_q_copy))
        late = send(*outs)
        out, w_k_new = out_own(pieces_of, w_o, pieces, factor, w_k_copy, [[e[s] for e in early] for s in (1, 2, 3)])
        for s in (1, 2, 3):
            out = lax.dynamic_update_slice(out, late[s][None], (cp ^ s, rows - 1, 0, 0))
        return out.reshape(hidden.shape), head_max, w_q_new, w_k_new

    return jax.shard_map(
        compute,
        mesh=mesh,
        in_specs=(P("dp", "cp", None), P("cp"), P(None, None), P(None, None), P(None, None), P(None, None)),
        out_specs=(P("dp", "cp", None), P(None), P(None, None), P(None, None)),
        check_vma=False,
    )
```
